32 devices in a mesh: gx: 4 (over y, x), gy: 2 (over core), gz: 4 (over z).
Axes of the slice: x: 2, y: 2, z: 4, core: 2. Of those that a mesh axis runs over, the one named last changes fastest.
Arguments:
- potential: float32 [240, 120, 512], P('gx', 'gy', 'gz'), may hold values from -6 to 6
- frag_root: int32 [3, 128], P(None, ('gx', 'gy', 'gz')), may hold values from 0 to 511, as said below
Outputs:
- frag_fields: float32 [128, 110592], P(('gx', 'gy', 'gz'))
The draws below stay inside these ranges and needn't reach their ends.
Inputs may be any that keep to these rules, and one draw needn't show every extreme that they name: `frag_root`: fragment f is held by the device of linear index f // 4 (gx slowest). Along each dimension the box's first cell is the start of a block plus an offset in [-34, B - 34), B being that dimension's cells of one device. Along y and z that block is the holding device's own; along x it is the block of some device with the same gy and gz index, the anchor. Every anchor of a device supplies exactly 1 of its fragments.
All inputs are finite; a program needn't handle non-finite values.
Results may differ from the reference program's by a relative error of at most 0.00007.
Values sent between devices are 32-bit elements; how exact they have to be, the bound alone decides.
A program may use at most 320 MiB of HBM per device.

```python
import math
import jax
import jax.numpy as jnp
from jax import lax

G = 48
CAP = 1
SLOTS = 4
BX = 60
BY = 60
BZ = 128
BOX = 68
HALO = 34
NX = 240
NY = 120
NZ = 512
N_GX = 4
N_GY = 2
N_GZ = 4


def draw_frag_root(key, part):
    subkeys = jax.random.split(jax.random.fold_in(key, 17), 6)
    devices = N_GX * N_GY * N_GZ
    pair_count = SLOTS // CAP
    favour = jax.random.randint(subkeys[0], (N_GX,), 0, 4) * 300
    jitter = jax.random.randint(subkeys[1], (devices, N_GX), 0, 1000)
    scores = (jitter + favour[None, :]) * N_GX + jnp.arange(N_GX, dtype=jnp.int32)[None, :]
    dummy_values, picked = lax.top_k(scores, pair_count)
    listed = jnp.repeat(picked.astype(jnp.int32), CAP, axis=1)
    shuffle_keys = jax.random.randint(subkeys[2], (devices, SLOTS), 0, 1000) * SLOTS + jnp.arange(SLOTS, dtype=jnp.int32)[None, :]
    shuffled = jnp.argsort(shuffle_keys, axis=1)
    anchors = jnp.take_along_axis(listed, shuffled, axis=1).reshape(-1)
    device = jnp.arange(devices * SLOTS, dtype=jnp.int32) // SLOTS
    row_y = device // N_GZ % N_GY
    row_z = device % N_GZ
    lowest = -HALO
    offset_x = jax.random.randint(subkeys[3], (devices * SLOTS,), lowest, BX - HALO)
    offset_y = jax.random.randint(subkeys[4], (devices * SLOTS,), lowest, BY - HALO)
    offset_z = jax.random.randint(subkeys[5], (devices * SLOTS,), lowest, BZ - HALO)
    offset_x = offset_x.at[0].set(lowest).at[1].set(BX - HALO - 1)
    offset_y = offset_y.at[0].set(lowest).at[1].set(BY - HALO - 1)
    offset_z = offset_z.at[0].set(lowest).at[1].set(BZ - HALO - 1)
    root_x = jnp.mod(anchors * BX + offset_x, BX * N_GX)
    root_y = jnp.mod(row_y * BY + offset_y, BY * N_GY)
    root_z = jnp.mod(row_z * BZ + offset_z, BZ * N_GZ)
    return jnp.stack([root_x, root_y, root_z]).astype(jnp.int32)


def steps_of(key, dims, pieces, smallest, top_value):
    level = 1.0
    for dim, shards_of in pieces:
        steps = jax.random.uniform(jax.random.fold_in(jax.random.fold_in(key, 6), dim), (shards_of,), jnp.float32, smallest / len(pieces), top_value / len(pieces))
        level = level * jnp.repeat(jnp.exp(steps), dims[dim] // shards_of).reshape((-1,) + (1,) * (len(dims) - 1 - dim))
    return level


def scatter_about(rng, dims, scale, most, shards=(), kind=jnp.bfloat16):
    array = scale * jax.random.normal(rng, dims, jnp.float32)
    if shards:
        array = array * steps_of(rng, dims, shards, -0.22, 0.18)
    return jnp.clip(array, -most, most).astype(kind)


def setup_inputs(seed: int = 0) -> dict:
    splits = jax.random.split(jax.random.key(seed), 3)
    potential = scatter_about(splits[0], (NX, NY, NZ), 1.0, 6.0, ((0, 4), (1, 2), (2, 4)), jnp.float32)
    frag_root = draw_frag_root(jax.random.fold_in(splits[2], 71), 0)
    return {"potential": potential, "frag_root": frag_root}


def interp_table(points, cells):
    row_index = jnp.arange(points, dtype=jnp.int32)[:, None]
    col_index = jnp.arange(cells, dtype=jnp.int32)[None, :]
    offset = row_index * cells - col_index * points
    period = points * cells
    summed = jnp.ones((points, cells), jnp.float32)
    for harmonic in range(1, points // 2):
        phase_angle = jnp.mod(harmonic * offset, period).astype(jnp.float32)
        summed = summed + 2.0 * jnp.cos((2.0 * math.pi / period) * phase_angle)
    return summed / cells


def refine(window, matrix):
    highest = lax.Precision.HIGHEST
    step_x = jnp.einsum('ax,xyz->ayz', matrix, window, precision=highest)
    step_y = jnp.einsum('by,ayz->abz', matrix, step_x, precision=highest)
    step_z = jnp.einsum('cz,abz->abc', matrix, step_y, precision=highest)
    return step_z.reshape(-1)


def reference(potential, frag_root):
    matrix = interp_table(G, BOX)
    wrapped = jnp.pad(potential, ((0, BOX), (0, BOX), (0, BOX)), mode="wrap")

    def single(corner):
        window = lax.dynamic_slice(wrapped, (corner[0], corner[1], corner[2]), (BOX, BOX, BOX))
        return refine(window, matrix)

    return lax.map(single, frag_root.T.astype(jnp.int32))
```

```python
import math

import jax
import jax.numpy as jnp
import numpy as np
from jax import lax
from jax.experimental import pallas as pl
from jax.experimental.pallas import tpu as pltpu
from jax.sharding import PartitionSpec as P

G = 48
BOX = 68
HALO = 34
LANES = 128
FOLD = LANES // HALO
BF = jnp.bfloat16
F32 = jnp.float32
MESH = pl.DeviceIdType.MESH
FAR = -1.0e6


def interp_values():
    offset = np.arange(G)[:, None] * BOX - np.arange(BOX)[None, :] * G
    summed = np.ones((G, BOX))
    for harmonic in range(1, G // 2):
        summed += 2.0 * np.cos(2.0 * math.pi / (G * BOX) * np.mod(harmonic * offset, G * BOX))
    return (summed / BOX).astype(np.float32)


def halves(value):
    high = value.astype(BF)
    return high, (value - high.astype(np.float32)).astype(BF)


def split(value):
    high = value.astype(BF)
    return high, (value - high.astype(F32)).astype(BF)


def octet_place(bx, i):
    c = i // 2
    odd = i % 2 == 1
    first = i < 2 * (HALO // 8)
    if isinstance(i, int):
        return (1, 8 * c) if odd else ((2, 8 * c) if first else (0, bx - HALO + 8 * (c - HALO // 8)))
    p = jnp.where(odd, 1, jnp.where(first, 2, 0))
    x0 = jnp.where(jnp.logical_or(odd, first), 8 * c, bx - HALO + 8 * (c - HALO // 8))
    return p, x0


def row_order(bx):
    octets = bx // 8 + 2 * (HALO // 8)
    rows = []
    for i in range(octets):
        p, x0 = octet_place(bx, i)
        rows += [(p, x0 + s) for s in range(8)]
    tail = [(0, x) for x in range(bx - HALO, bx)] + [(1, x) for x in range(bx)] + [(2, x) for x in range(HALO)]
    tail = [t for t in tail if t not in rows]
    assert len(tail) == 8 and len(set(rows + tail)) == len(rows) + 8
    return rows + tail, octets


def tables(bx, by, n, ny, slots):
    high, low = halves(interp_values())
    tab = np.zeros((2 * G, LANES), BF)
    tab[:G, :BOX], tab[G:, :BOX] = high, low
    tabt = np.zeros((LANES, 2 * LANES), BF)
    tabt[:BOX, :G], tabt[:BOX, LANES:LANES + G] = high.T, low.T
    tabi = np.zeros((2, G, slots, slots, LANES), BF)
    for f in range(slots):
        tabi[0, :, f, f, :BOX], tabi[1, :, f, f, :BOX] = high, low
    tabi = tabi.reshape(2 * G * slots, slots * LANES)
    rows, _ = row_order(bx)
    part = np.array([p for p, x in rows])
    ext = np.array([x - (bx - HALO) + (0, bx, 2 * bx)[p] for p, x in rows])
    cols = np.zeros((8, n * len(rows)), np.float32)
    cols[0] = np.tile(ext, n)
    cols[1] = np.tile(part - 1, n) - np.repeat(np.arange(n), len(rows))
    return tab, tabt, tabi, cols


def stages(bx, octets):
    step = 4 * FOLD
    ends = [min(step * (s + 1), bx) for s in range(-(-bx // step))]
    need = [octet_place(bx, i)[1] + 8 for i in range(octets)]
    plan, i = [], 0
    for s, end in enumerate(ends):
        start = i
        while i < octets and need[i] <= end:
            i += 1
        plan.append((step * s, end, start, i))
    return plan


def fused_kernel(info, pot, roots, tab, tabt, tabi, cols, got, mx, peer, pack, zin, zpeer, rt, yb, lhs, wz, us,
                 outb, raw_s, raw_r, z_s, z_r, rel_s, rel_r, rt_s, rt_r, gx_s, gx_r, own_s):
    n, ny, nz, slots = info
    bx, by, bz = pot.shape
    total_x, total_y, total_z = bx * n, by * ny, bz * nz
    rows, octets = row_order(bx)
    plan = stages(bx, octets)
    pad = yb.shape[1] // (2 * ny)
    half = ny * pad
    ix, iy, iz = lax.axis_index("gx"), lax.axis_index("gy"), lax.axis_index("gz")
    mate = {"gy": lax.rem(iy + 1, ny)}
    above = {"gz": lax.rem(iz + 1, nz)}
    below = {"gz": lax.rem(iz + nz - 1, nz)}
    holder = [{"gx": lax.rem(ix + n - j, n)} for j in range(n)]

    def copy(src, dst, ss, rs, where):
        return pltpu.make_async_remote_copy(
            src_ref=src, dst_ref=dst, send_sem=ss, recv_sem=rs, device_id=where, device_id_type=MESH)

    barrier = pltpu.get_barrier_semaphore()
    friends = [mate, above, below] + holder[1:]
    for where in friends:
        pl.semaphore_signal(barrier, inc=1, device_id=where, device_id_type=MESH)
    pl.semaphore_wait(barrier, len(friends))

    root_copy = [None] + [copy(roots, rt.at[j], rt_s.at[j], rt_r.at[j],
                               {"gx": lax.rem(ix + j, n)}) for j in range(1, n)]
    raw, zc, rel = [], [], []
    for s, (x0, x1, _, _) in enumerate(plan):
        xs = slice(x0, x1)
        rs = slice(x0 // FOLD, x1 // FOLD)
        raw.append(copy(pot.at[xs], peer.at[xs], raw_s.at[s], raw_r.at[s], mate))
        zc.append([copy(pack.at[side, rs], zin.at[side, rs], z_s.at[side, s], z_r.at[side, s], where)
                   for side, where in ((0, above), (1, below))])
        rel.append([copy(zin.at[side, rs], zpeer.at[side, rs], rel_s.at[side, s], rel_r.at[side, s], mate)
                    for side in (0, 1)])

    lane_p = lax.broadcasted_iota(jnp.int32, (by, LANES), 1)

    def pack_rows(x0, x1):
        def one(r, carry):
            down = jnp.zeros((by, LANES), F32)
            up = down
            for g in range(FOLD):
                v = pot[FOLD * r + g]
                mine = jnp.logical_and(lane_p >= g * HALO, lane_p < (g + 1) * HALO)
                down = jnp.where(mine, pltpu.roll(v, ((g + 1) * HALO) % LANES, 1), down)
                up = jnp.where(mine, pltpu.roll(v, g * HALO, 1) if g else v, up)
            pack[0, r] = down
            pack[1, r] = up
            return carry
        lax.fori_loop(x0 // FOLD, x1 // FOLD, one, 0)

    last = len(plan) - 1
    for s, (x0, x1, _, _) in enumerate(plan):
        pack_rows(x0, x1)
        raw[s].start()
        if s:
            for c in zc[s - 1]:
                c.start()
    for j in range(1, n):
        root_copy[j].start()
    for c in zc[last]:
        c.start()

    lane_r = lax.broadcasted_iota(jnp.int32, (1, LANES), 1)
    fix, fiy, fiz = ix.astype(F32), iy.astype(F32), iz.astype(F32)

    def wrapped(v, period):
        v = jnp.where(v < 0, v + period, v)
        return jnp.where(v >= period, v - period, v)

    def lane_sum(v):
        return jnp.sum(v, axis=1, keepdims=True)

    ye = lax.broadcasted_iota(jnp.int32, (1, half), 1)
    block_y = jnp.zeros((1, half), jnp.int32)
    for c in range(1, ny):
        block_y = block_y + (ye >= c * pad).astype(jnp.int32)
    real_y = ye - block_y * pad < by
    cells_y = jnp.where(real_y, (ye - block_y * (pad - by)).astype(F32), FAR)
    ze = lax.broadcasted_iota(jnp.int32, (2 * LANES, 1), 0)
    zf = ze.astype(F32)
    cells_z = jnp.where(ze < bz + HALO, zf + HALO, jnp.where(ze < bz + 2 * HALO, zf - (bz + HALO), FAR))
    sub_x = lax.broadcasted_iota(jnp.int32, (LANES, half), 0).astype(F32)
    lane_x = lax.broadcasted_iota(jnp.int32, (2 * LANES, LANES), 1).astype(F32)
    dot = lambda a, b: jnp.dot(a, b, preferred_element_type=F32)

    def matrices(j, source):
        rx, ry, rz = source[0:1, :], source[1:2, :], source[2:3, :]
        xm = wrapped(rx + HALO, total_x)
        ys = wrapped(ry - fiy * by, total_y)
        zs = wrapped(rz + HALO - fiz * bz, total_z)
        for p in range(3):
            target = wrapped(fix + (1 - p), n) * bx
            hit = jnp.logical_and(lane_r < slots, jnp.logical_and(xm >= target, xm < target + bx))
            some = lane_sum(jnp.where(hit, 1.0, 0.0)) > 0.5
            sy = lane_sum(jnp.where(hit, ys, 0.0))
            sz = lane_sum(jnp.where(hit, zs, 0.0))
            place = jnp.where(some, cells_y - sy, FAR)
            place = jnp.where(jnp.logical_and(place < 0, place > FAR / 2), place + total_y, place)
            hot = jnp.where(sub_x == place, 1.0, 0.0).astype(BF)
            m = dot(tab[...], hot).astype(BF)
            lhs[p, j * G:(j + 1) * G, :half] = m[:G]
            lhs[p, j * G:(j + 1) * G, half:2 * half] = m[:G]
            lhs[p, j * G:(j + 1) * G, 2 * half:] = m[G:]
            place = jnp.where(some, cells_z - sz, FAR)
            hot = jnp.where(lane_x == place, 1.0, 0.0).astype(BF)
            wz[j, p] = dot(hot, tabt[...]).astype(BF)

    matrices(0, roots)
    xm = wrapped(roots[0:1, :] + HALO, total_x)
    hots = []
    sub_w = lax.broadcasted_iota(jnp.int32, (LANES, n * len(rows)), 0).astype(F32)
    ext, src = cols[0:1, :], cols[1:2, :]
    for f in range(slots):
        mine = lane_sum(jnp.where(lane_r == f, xm, 0.0))
        slab = jnp.zeros((1, 1), F32)
        for k in range(1, n):
            slab = slab + jnp.where(mine >= k * bx, 1.0, 0.0)
        t = src + (slab - fix)
        good = jnp.logical_or(t == 0, jnp.logical_or(t == n, t == -n))
        place = jnp.where(good, ext - (mine - slab * bx), FAR)
        hots.append(jnp.where(sub_w == place, 1.0, 0.0).astype(BF))
    mx[...] = dot(tabi[...], jnp.concatenate(hots, axis=0)).astype(BF)
    for j in range(1, n):
        root_copy[j].wait_recv()
        matrices(j, rt.at[j])

    lane_h = lax.broadcasted_iota(jnp.int32, (pad, LANES), 1)
    blank = jnp.zeros((pad - by, LANES), F32)

    def full(v):
        return jnp.concatenate([v, blank], axis=0)

    def slab_rows(x0, x1):
        def one(r, carry):
            for c, (block, halos) in enumerate(((pot, zin), (peer, zpeer))):
                down = full(halos[0, r])
                up = full(halos[1, r])
                for g in range(FOLD):
                    x = FOLD * r + g
                    a = pltpu.roll(up, (-g * HALO) % LANES, 1) if g else up
                    b = pltpu.roll(down, (HALO - g * HALO) % LANES, 1) if g != 1 else down
                    second = jnp.where(lane_h < HALO, a, jnp.where(lane_h < 2 * HALO, b, 0.0))
                    for side, v in ((0, full(block[x])), (1, second)):
                        h, l = split(v)
                        lanes = slice(side * LANES, (side + 1) * LANES)
                        yb[x, c * pad:(c + 1) * pad, lanes] = h
                        yb[x, half + c * pad:half + (c + 1) * pad, lanes] = l
            return carry
        lax.fori_loop(x0 // FOLD, x1 // FOLD, one, 0)

    def row(p, x, s):
        r = dot(lhs[p, :, :2 * half], yb[x]) + dot(lhs[p, :, 2 * half:], yb[x, :half])
        us[:, s, :] = r

    def finish(j, p):
        h, l = split(us[j * G:(j + 1) * G].reshape(G * 8, us.shape[2]))
        a = dot(h, wz[j, p])
        return a[:, :LANES] + a[:, LANES:] + dot(l, wz[j, p, :, :LANES])

    def store(j, i, r):
        at = pl.multiple_of(8 * i, 8)
        for b in range(G):
            outb[j, pl.ds(at, 8), b * G:(b + 1) * G] = r[8 * b:8 * b + 8, :G]

    def sent(j, i):
        at = pl.ds(pl.multiple_of(8 * i, 8), 8)
        return copy(outb.at[j, at], got.at[j, at], gx_s.at[j, i], gx_r.at[j, i], holder[j])

    def emit(i, value):
        previous = None
        for j in list(range(1, n)) + [0]:
            store(j, i, value(j))
            if previous:
                sent(previous, i).start()
            previous = j

    def octet(i, carry):
        p, x0 = octet_place(bx, i)
        for s in range(8):
            row(p, x0 + s, s)
        emit(i, lambda j: finish(j, p))
        return carry

    for c in zc[0]:
        c.wait_recv()
    for c in rel[0]:
        c.start()
    for s, (x0, x1, i0, i1) in enumerate(plan):
        raw[s].wait_recv()
        for c in rel[s]:
            c.wait_recv()
        slab_rows(x0, x1)
        lax.fori_loop(i0, i1 - 1, octet, 0)
        if s < last:
            for c in zc[s + 1]:
                c.wait_recv()
            for c in rel[s + 1]:
                c.start()
        octet(i1 - 1, 0)

    tail = rows[8 * octets:]
    for s, (p, x) in enumerate(tail):
        row(p, x, s)
    sub = lax.broadcasted_iota(jnp.int32, (G * 8, LANES), 0) % 8

    def tail_value(j):
        total = jnp.zeros((G * 8, LANES), F32)
        for p in range(3):
            places = [s for s, t in enumerate(tail) if t[0] == p]
            mine = jnp.logical_and(sub >= places[0], sub <= places[-1])
            total = jnp.where(mine, finish(j, p), total)
        return total

    emit(octets, tail_value)
    own = pltpu.make_async_copy(outb.at[0], got.at[0], own_s)
    own.start()
    for s in range(last + 1):
        raw[s].wait_send()
        for c in zc[s] + rel[s]:
            c.wait_send()
    for j in range(1, n):
        root_copy[j].wait_send()

    def finished(i, carry):
        for j in range(1, n):
            sent(j, i).wait()
        return carry

    lax.fori_loop(0, octets + 1, finished, 0)
    own.wait()


def fused(info, pot, roots, consts):
    n, ny, nz, slots = info
    bx, by, bz = pot.shape
    rows, octets = row_order(bx)
    count = len(rows)
    chunks = len(stages(bx, octets))
    pad = -(-by // 16) * 16
    half = ny * pad
    dma = pltpu.SemaphoreType.DMA
    vmem = pl.BlockSpec(memory_space=pltpu.VMEM)
    folded = (2, bx // FOLD, by, LANES)
    return pl.pallas_call(
        lambda *refs: fused_kernel(info, *refs),
        in_specs=[vmem] * 6,
        out_specs=[pl.BlockSpec(memory_space=pl.ANY), vmem],
        out_shape=[jax.ShapeDtypeStruct((n, count, G * G), F32),
                   jax.ShapeDtypeStruct((2 * G * slots, n * count), BF)],
        scratch_shapes=[
            pltpu.VMEM((bx, by, LANES), F32),
            pltpu.VMEM(folded, F32),
            pltpu.VMEM(folded, F32),
            pltpu.VMEM(folded, F32),
            pltpu.VMEM((n, 8, LANES), F32),
            pltpu.VMEM((bx, 2 * half, 2 * LANES), BF),
            pltpu.VMEM((3, n * G, 3 * half), BF),
            pltpu.VMEM((n, 3, 2 * LANES, 2 * LANES), BF),
            pltpu.VMEM((n * G, 8, 2 * LANES), F32),
            pltpu.VMEM((n, count, G * G), F32),
            dma((chunks,)), dma((chunks,)),
            dma((2, chunks)), dma((2, chunks)),
            dma((2, chunks)), dma((2, chunks)),
            dma((n,)), dma((n,)),
            dma((n, octets + 1)), dma((n, octets + 1)),
            dma,
        ],
        compiler_params=pltpu.CompilerParams(
            collective_id=0, has_side_effects=True, vmem_limit_bytes=60 * 1024 * 1024),
        cost_estimate=pl.CostEstimate(flops=24 * 10 ** 9, bytes_accessed=16 * 1024 * 1024, transcendentals=0),
        name="exchange_contract",
    )(pot, roots, *consts)


def last_kernel(n, slots, mx, got, out):
    t = pl.program_id(0)
    count, width = got.shape[1], got.shape[2]
    m = G * slots
    dot = lambda a, b: jnp.dot(a, b, preferred_element_type=F32)
    total = None
    for j in range(n):
        h, l = split(got[j])
        both = mx[:, j * count:(j + 1) * count]
        a = dot(both, h)
        term = a[:m] + a[m:] + dot(both[:m], l)
        total = term if total is None else total + term
    for a in range(G):
        at = pl.multiple_of(a * G * G + t * width, LANES)
        out[:, pl.ds(at, width)] = total[a * slots:(a + 1) * slots]


def last(info, mx, got):
    n, ny, nz, slots = info
    count = got.shape[1]
    width = 2 * LANES
    return pl.pallas_call(
        lambda *refs: last_kernel(n, slots, *refs),
        grid=(G * G // width,),
        in_specs=[pl.BlockSpec(mx.shape, lambda t: (0, 0)),
                  pl.BlockSpec((n, count, width), lambda t: (0, 0, t))],
        out_specs=pl.BlockSpec((slots, G ** 3), lambda t: (0, 0)),
        out_shape=jax.ShapeDtypeStruct((slots, G ** 3), F32),
        compiler_params=pltpu.CompilerParams(vmem_limit_bytes=60 * 1024 * 1024),
        name="contract_x",
    )(mx, got)


def body(potential, frag_root):
    bx, by, bz = potential.shape
    n, ny, nz = lax.axis_size("gx"), lax.axis_size("gy"), lax.axis_size("gz")
    slots = frag_root.shape[1]
    info = (n, ny, nz, slots)
    roots = jnp.pad(frag_root.astype(F32), ((0, 5), (0, LANES - slots)))
    consts = [jnp.asarray(c) for c in tables(bx, by, n, ny, slots)]
    got, mx = fused(info, potential, roots, consts)
    return last(info, mx, got)


def solution(mesh):
    return jax.shard_map(
        body,
        mesh=mesh,
        in_specs=(P("gx", "gy", "gz"), P(None, ("gx", "gy", "gz"))),
        out_specs=P(("gx", "gy", "gz"), None),
        check_vma=False,
    )
```

```python
import math

import jax
import jax.numpy as jnp
import numpy as np
from jax import lax
from jax.experimental import pallas as pl
from jax.experimental.pallas import tpu as pltpu
from jax.sharding import PartitionSpec as P

G = 48
BOX = 68
HALO = 34
LANES = 128
FOLD = LANES // HALO
BF = jnp.bfloat16
F32 = jnp.float32
MESH = pl.DeviceIdType.MESH
FAR = -1.0e6
FAR_CELL = -(1 << 20)
STEPS = 4
HIGH = lax.Precision.HIGH


def interp_values():
    offset = np.arange(G)[:, None] * BOX - np.arange(BOX)[None, :] * G
    summed = np.ones((G, BOX))
    for harmonic in range(1, G // 2):
        summed += 2.0 * np.cos(2.0 * math.pi / (G * BOX) * np.mod(harmonic * offset, G * BOX))
    return (summed / BOX).astype(np.float32)


def halves(value):
    high = value.astype(BF)
    return high, (value - high.astype(np.float32)).astype(BF)


def split(value):
    high = value.astype(BF)
    return high, (value - high.astype(F32)).astype(BF)


def shift(array, axis, step):
    devices = lax.axis_size(axis)
    return lax.ppermute(array, axis, [(i, (i + step) % devices) for i in range(devices)])


def placed(start, cells, period, valid):
    place = cells - start[..., None]
    if period:
        place = jnp.mod(place, period)
    inside = jnp.logical_and(place >= 0, place < BOX)
    inside = jnp.logical_and(inside, valid[..., None])
    base = jnp.asarray(interp_values())
    index = jnp.where(inside, place, BOX)
    hot = (index[..., None, :] == jnp.arange(BOX, dtype=jnp.int32)[:, None]).astype(jnp.float32)
    return jnp.einsum("ax,...xe->...ae", base, hot, precision=lax.Precision.HIGHEST)


def pack_kernel(pot, low, high):
    rows, by = pot.shape[1], pot.shape[2]
    lane = lax.broadcasted_iota(jnp.int32, (rows * by, LANES), 1)
    down = jnp.zeros((rows * by, LANES), F32)
    up = down
    for g in range(FOLD):
        v = pot[g].reshape(rows * by, LANES)
        mine = jnp.logical_and(lane >= g * HALO, lane < (g + 1) * HALO)
        down = jnp.where(mine, pltpu.roll(v, ((g + 1) * HALO) % LANES, 1), down)
        up = jnp.where(mine, pltpu.roll(v, g * HALO, 1) if g else v, up)
    low[...] = down.reshape(rows, by, LANES)
    high[...] = up.reshape(rows, by, LANES)


def pack(pot):
    fold, rows, by, bz = pot.shape
    step = rows // STEPS
    spec = pl.BlockSpec((step, by, LANES), lambda i: (i, 0, 0))
    shape = jax.ShapeDtypeStruct((rows, by, LANES), F32)
    return pl.pallas_call(
        pack_kernel,
        grid=(STEPS,),
        in_specs=[pl.BlockSpec((fold, step, by, LANES), lambda i: (0, i, 0, 0))],
        out_specs=[spec, spec],
        out_shape=[shape, shape],
        cost_estimate=pl.CostEstimate(flops=0, bytes_accessed=4 * pot.size * 2, transcendentals=0),
        name="pack_halos",
    )(pot)


def plain_slab_kernel(ny, *refs):
    owns, lows, highs, out = refs[:ny], refs[ny:2 * ny], refs[2 * ny:3 * ny], refs[3 * ny]
    rows, by = owns[0].shape[1], owns[0].shape[2]
    pad = out.shape[2] // (2 * ny)
    half = ny * pad
    lane = lax.broadcasted_iota(jnp.int32, (pad, LANES), 1)
    blank = jnp.zeros((pad - by, LANES), F32)

    def full(v):
        return jnp.concatenate([v, blank], axis=0)

    for c in range(ny):
        for r in range(rows):
            up = full(highs[c][r])
            down = full(lows[c][r])
            for g in range(FOLD):
                first = full(owns[c][g, r])
                a = pltpu.roll(up, (-g * HALO) % LANES, 1) if g else up
                b = pltpu.roll(down, (HALO - g * HALO) % LANES, 1) if g != 1 else down
                second = jnp.where(lane < HALO, a, jnp.where(lane < 2 * HALO, b, 0.0))
                for side, v in ((0, first), (1, second)):
                    h, l = split(v)
                    cols = slice(side * LANES, (side + 1) * LANES)
                    out[g, r, c * pad:(c + 1) * pad, cols] = h
                    out[g, r, half + c * pad:half + (c + 1) * pad, cols] = l


def slabs(owns, lows, highs):
    ny = len(owns)
    fold, rows, by, bz = owns[0].shape
    pad = -(-by // 16) * 16
    step = rows // STEPS
    big = pl.BlockSpec((fold, step, by, LANES), lambda i: (0, i, 0, 0))
    small = pl.BlockSpec((step, by, LANES), lambda i: (i, 0, 0))
    return pl.pallas_call(
        lambda *refs: plain_slab_kernel(ny, *refs),
        grid=(STEPS,),
        in_specs=[big] * ny + [small] * (2 * ny),
        out_specs=pl.BlockSpec((fold, step, 2 * ny * pad, 2 * LANES), lambda i: (0, i, 0, 0)),
        out_shape=jax.ShapeDtypeStruct((fold, rows, 2 * ny * pad, 2 * LANES), BF),
        cost_estimate=pl.CostEstimate(flops=0, bytes_accessed=16 * 1024 * 1024, transcendentals=0),
        name="build_slabs",
    )(*owns, *lows, *highs)


def contract_kernel(bx, yb, my, mz, out, lhs, wz, us):
    k = my.shape[2]
    for p in range(3):
        h, l = split(my[p])
        lhs[p, :G, :k] = h
        lhs[p, :G, k:] = h
        lhs[p, G:, :k] = l
        lhs[p, G:, k:] = jnp.zeros_like(l)
        h, l = split(mz[p])
        wz[p, 0] = h
        wz[p, 1] = l
    nl, nm = HALO // 8, bx // 8

    def row(p, x, s):
        r = jnp.dot(lhs[p], yb[x], preferred_element_type=F32)
        us[:, s, :] = r[:G] + r[G:]

    def finish(p):
        h, l = split(us[...].reshape(G * 8, us.shape[2]))
        dot = lambda a, b: jnp.dot(a, b, preferred_element_type=F32)
        return dot(h, wz[p, 0]) + dot(h, wz[p, 1]) + dot(l, wz[p, 0])

    def store(r, row0):
        for b in range(G):
            out[pl.ds(row0, 8), b * G:(b + 1) * G] = r[8 * b:8 * b + 8]

    def block(i, carry):
        p = (i >= nl).astype(jnp.int32) + (i >= nl + nm).astype(jnp.int32)
        x0 = jnp.where(p == 0, bx - HALO + 8 * i, jnp.where(p == 1, 8 * (i - nl), 8 * (i - nl - nm)))
        for s in range(8):
            row(p, x0 + s, s)
        store(finish(p), pl.multiple_of(8 * i, 8))
        return carry

    blocks = 2 * nl + nm
    lax.fori_loop(0, blocks, block, 0)
    tail = plain_tail_rows(bx)
    for s, (p, x) in enumerate(tail):
        row(p, x, s)
    sub = lax.broadcasted_iota(jnp.int32, (G * 8, G), 0) % 8
    total = jnp.zeros((G * 8, G), F32)
    for p in range(3):
        places = [s for s, t in enumerate(tail) if t[0] == p]
        mine = jnp.logical_and(sub >= places[0], sub <= places[-1])
        total = jnp.where(mine, finish(p), total)
    store(total, 8 * blocks)


def plain_tail_rows(bx):
    nl, nm = HALO // 8 * 8, bx // 8 * 8
    rows = [(0, bx - HALO + x) for x in range(nl, HALO)]
    rows += [(1, x) for x in range(nm, bx)]
    rows += [(2, x) for x in range(nl, HALO)]
    assert len(rows) == 8
    return rows


def plain_row_order(bx):
    nl, nm = HALO // 8 * 8, bx // 8 * 8
    rows = [(0, bx - HALO + x) for x in range(nl)] + [(1, x) for x in range(nm)]
    return rows + [(2, x) for x in range(nl)] + plain_tail_rows(bx)


def contract(bx, yb, my, mz):
    rows = len(plain_row_order(bx))
    k = my.shape[2]
    width = yb.shape[2]
    return pl.pallas_call(
        lambda *refs: contract_kernel(bx, *refs),
        in_specs=[pl.BlockSpec(memory_space=pltpu.VMEM)] * 3,
        out_specs=pl.BlockSpec(memory_space=pltpu.VMEM),
        out_shape=jax.ShapeDtypeStruct((rows, G * G), F32),
        scratch_shapes=[
            pltpu.VMEM((3, 2 * G, 2 * k), BF),
            pltpu.VMEM((3, 2, width, G), BF),
            pltpu.VMEM((G, 8, width), F32),
        ],
        compiler_params=pltpu.CompilerParams(vmem_limit_bytes=40 * 1024 * 1024),
        cost_estimate=pl.CostEstimate(
            flops=6 * 10 ** 9, bytes_accessed=2 * yb.size + 4 * rows * G * G, transcendentals=0),
        name="contract_yz",
    )(yb, my, mz)


def plain_body(potential, frag_root):
    bx, by, bz = potential.shape
    n = lax.axis_size("gx")
    ny = lax.axis_size("gy")
    nz = lax.axis_size("gz")
    ix, iy, iz = lax.axis_index("gx"), lax.axis_index("gy"), lax.axis_index("gz")
    total_x, total_y, total_z = bx * n, by * ny, bz * nz
    slots = frag_root.shape[1]

    folded = potential.reshape(FOLD, bx // FOLD, by, bz)
    low, high = pack(folded)
    low = shift(low, "gz", 1)
    high = shift(high, "gz", -1)
    owns = [folded] + [shift(folded, "gy", -j) for j in range(1, ny)]
    lows = [low] + [shift(low, "gy", -j) for j in range(1, ny)]
    highs = [high] + [shift(high, "gy", -j) for j in range(1, ny)]
    root = jnp.stack([frag_root] + [shift(frag_root, "gx", j) for j in range(1, n)])
    yb = slabs(owns, lows, highs)
    yb = yb.reshape(bx, yb.shape[2], yb.shape[3])

    anchor = jnp.mod(root[:, 0] + HALO, total_x) // bx
    start_y = jnp.mod(root[:, 1] - iy * by, total_y)
    start_z = jnp.mod(root[:, 2] + HALO - iz * bz, total_z)
    pad = -(-by // 16) * 16
    e = jnp.arange(ny * pad, dtype=jnp.int32)
    cells_y = e // pad * by + e % pad
    real_y = e % pad < by
    e = jnp.arange(2 * LANES, dtype=jnp.int32)
    cells_z = jnp.where(e < bz + HALO, e + HALO, jnp.where(e < bz + 2 * HALO, e - bz - HALO, FAR_CELL))
    delta = jnp.array([1, 0, -1], jnp.int32)
    hit = anchor[:, None, :] == jnp.mod(ix + delta, n)[None, :, None]
    valid = jnp.any(hit, axis=2)
    pick = lambda v: jnp.sum(jnp.where(hit, v[:, None, :], 0), axis=2)
    my = placed(pick(start_y), cells_y, total_y, valid)
    my = jnp.where(real_y, my, 0.0)
    mz = placed(pick(start_z), cells_z, None, valid).transpose(0, 1, 3, 2)

    order = [j for j in range(2, n, 2)] + [j for j in range(n) if j % 2]
    got = [None] * n
    for j in order:
        got[j] = shift(contract(bx, yb, my[j], mz[j]), "gx", -j)
    got[0] = contract(bx, yb, my[0], mz[0])

    mine = jnp.mod(frag_root[0] + HALO, total_x)
    slab = mine // bx
    rel = mine - slab * bx
    rows = plain_row_order(bx)
    part = jnp.array([p for p, x in rows], jnp.int32)
    ext = jnp.array([x - (bx - HALO) if p == 0 else x + HALO + (p - 1) * bx for p, x in rows], jnp.int32)
    mx = placed(rel, ext, None, jnp.ones((slots,), bool))
    source = jnp.mod(slab[:, None] - ix + part[None, :] - 1, n)
    fields = None
    for j in [0] + order:
        m = jnp.where((source == j)[:, None, :], mx, 0.0).reshape(slots * G, -1)
        term = jnp.dot(m, got[j], precision=HIGH)
        fields = term if fields is None else fields + term
    return fields.reshape(slots, -1)


def octet_place(bx, i):
    c = i // 2
    odd = i % 2 == 1
    first = i < 2 * (HALO // 8)
    if isinstance(i, int):
        return (1, 8 * c) if odd else ((2, 8 * c) if first else (0, bx - HALO + 8 * (c - HALO // 8)))
    p = jnp.where(odd, 1, jnp.where(first, 2, 0))
    x0 = jnp.where(jnp.logical_or(odd, first), 8 * c, bx - HALO + 8 * (c - HALO // 8))
    return p, x0


def layout(bx):
    octets = bx // 8 + 2 * (HALO // 8)
    placed_rows = [(p, x0 + s) for p, x0 in (octet_place(bx, i) for i in range(octets)) for s in range(8)]
    tail = [(0, x) for x in range(bx - HALO, bx)] + [(1, x) for x in range(bx)] + [(2, x) for x in range(HALO)]
    tail = [t for t in tail if t not in placed_rows]
    assert len(tail) == 8 and len(set(placed_rows + tail)) == len(placed_rows) + 8
    sides = [t for i in range(0, octets + 1, 2) for t in placed_rows[8 * i:8 * i + 8] if t[0] != 1]
    mids = [t for t in placed_rows if t[0] == 1]
    assert len(sides) == SIDES and len(mids) + 8 == MIDS
    return sides, mids, tail, octets


SIDES = 2 * (HALO // 8) * 8
MIDS = 64
BLOCK = SIDES + 64
CHUNKS = (3, 4, 3, 2, 2, 2)


def tables(bx, n, slots):
    high, low = halves(interp_values())
    tab = np.zeros((2 * G, LANES), BF)
    tab[:G, :BOX], tab[G:, :BOX] = high, low
    tabt = np.zeros((LANES, 2 * LANES), BF)
    tabt[:BOX, :G], tabt[:BOX, LANES:LANES + G] = high.T, low.T
    tabi = np.zeros((2, G, slots, slots, LANES), BF)
    for f in range(slots):
        tabi[0, :, f, f, :BOX], tabi[1, :, f, f, :BOX] = high, low
    tabi = tabi.reshape(2 * G * slots, slots * LANES)
    sides, mids, tail, _ = layout(bx)
    reach = lambda p, x: x - (bx - HALO) + (0, bx, 2 * bx)[p]
    cols = np.full((8, 2 * n * 64), FAR, np.float32)
    for j in range(n):
        for half, rows in ((0, sides), (1, [t if t[0] != 1 else None for t in tail])):
            for r, t in enumerate(rows):
                if t:
                    cols[0:2, half * n * 64 + j * 64 + r] = reach(*t), t[0] - 1
        for half in (0, 1):
            cols[2, half * n * 64 + j * 64:half * n * 64 + (j + 1) * 64] = j
        for a in range(G):
            cols[3, n * 64 + j * 64 + 8 + a] = a
    for r, t in enumerate(mids + tail):
        if t[0] == 1:
            cols[4, r] = cols[4, MIDS + r] = reach(*t)
    return tab, tabt, tabi, cols


def stages(bx, octets):
    need = [octet_place(bx, i)[1] + 8 for i in range(octets)]
    plan, i, t = [], 0, 0
    for count in CHUNKS:
        start, end = i, t + count
        x0, x1 = min(t * LANES // HALO, bx), min(end * LANES // HALO, bx)
        while i < octets and need[i] <= x1:
            i += 1
        plan.append((x0, x1, start, i, t, end))
        t = end
    assert x1 == bx and t == tiles_of(bx) and i == octets
    return plan


def tiles_of(bx):
    return -(-bx * HALO // LANES)


def fused_kernel(info, pot_hbm, own_root, tab, tabt, tabi, cols, out, pot, got, mx, peer, pack, zin, zpeer, rt, yb,
                 lhs, wz, us, outb, mids, ma, acc, load_s, raw_s, raw_r, z_s, z_r, rel_s, rel_r, rt_s, rt_r,
                 gx_s, gx_r):
    n, ny, nz, slots = info
    bx, by, bz = pot.shape
    total_x, total_y, total_z = bx * n, by * ny, bz * nz
    side_rows, mid_rows, tail, octets = layout(bx)
    plan = stages(bx, octets)
    last = len(plan) - 1
    pad = yb.shape[1] // (2 * ny)
    half = ny * pad
    ix, iy, iz = lax.axis_index("gx"), lax.axis_index("gy"), lax.axis_index("gz")
    mate = {"gy": lax.rem(iy + 1, ny)}
    above = {"gz": lax.rem(iz + 1, nz)}
    below = {"gz": lax.rem(iz + nz - 1, nz)}
    spot = [ix, ix + 1 - 2 * lax.rem(ix, 2), lax.rem(ix + 2, 4), 3 - ix]
    other = [{"gx": d} for d in spot]
    order = [3, 1, 2]
    bank = [3, 0, 1, 2]

    def copy(src, dst, ss, rs, where):
        return pltpu.make_async_remote_copy(
            src_ref=src, dst_ref=dst, send_sem=ss, recv_sem=rs, device_id=where, device_id_type=MESH)

    load = pltpu.make_async_copy(pot_hbm, pot, load_s)
    load.start()
    barrier = pltpu.get_barrier_semaphore()
    friends = [above, below, mate] + other[1:]
    for where in friends:
        pl.semaphore_signal(barrier, inc=1, device_id=where, device_id_type=MESH)

    root_copy = [None] + [copy(rt.at[0], rt.at[j], rt_s.at[j], rt_r.at[j], other[j]) for j in range(1, n)]
    raw, zc, rel = [], [], []
    for s, (x0, x1, _, _, t0, t1) in enumerate(plan):
        xs = slice(x0, x1)
        rs = slice(t0, t1)
        raw.append(copy(pot.at[xs], peer.at[xs], raw_s.at[s], raw_r.at[s], mate))
        zc.append([copy(pack.at[side, rs], zin.at[side, rs], z_s.at[side, s], z_r.at[side, s], where)
                   for side, where in ((0, above), (1, below))])
        rel.append([copy(zin.at[side, rs], zpeer.at[side, rs], rel_s.at[side, s], rel_r.at[side, s], mate)
                    for side in (0, 1)])

    lane_p = lax.broadcasted_iota(jnp.int32, (by, LANES), 1)

    def pack_tile(t, carry):
        down = jnp.zeros((by, LANES), F32)
        up = down
        x0 = LANES * t // HALO
        for k in range(-(-LANES // HALO) + 1):
            x = jnp.minimum(x0 + k, bx - 1)
            at = HALO * x - LANES * t
            v = pot[x]
            mine = jnp.logical_and(lane_p >= at, lane_p < at + HALO)
            down = jnp.where(mine, pltpu.roll(v, lax.rem(at + HALO + LANES, LANES), 1), down)
            up = jnp.where(mine, pltpu.roll(v, lax.rem(at + LANES, LANES), 1), up)
        pack[0, t] = down
        pack[1, t] = up
        return carry

    rt[0] = jnp.zeros(rt.shape[1:], F32)
    rt[0, :3, :slots] = own_root[...].astype(F32)
    load.wait()
    lax.fori_loop(0, tiles_of(bx), pack_tile, 0)
    pl.semaphore_wait(barrier, len(friends))
    for s in range(last + 1):
        for c in zc[s]:
            c.start()
        raw[s].start()
        if s == 0:
            for j in range(1, n):
                root_copy[j].start()

    lane_r = lax.broadcasted_iota(jnp.int32, (1, LANES), 1)
    fiy, fiz = iy.astype(F32), iz.astype(F32)
    fspot = [d.astype(F32) for d in spot]

    def wrapped(v, period):
        v = jnp.where(v < 0, v + period, v)
        return jnp.where(v >= period, v - period, v)

    def lane_sum(v):
        return jnp.sum(v, axis=1, keepdims=True)

    ye = lax.broadcasted_iota(jnp.int32, (1, half), 1)
    block_y = jnp.zeros((1, half), jnp.int32)
    for c in range(1, ny):
        block_y = block_y + (ye >= c * pad).astype(jnp.int32)
    real_y = ye - block_y * pad < by
    cells_y = jnp.where(real_y, (ye - block_y * (pad - by)).astype(F32), FAR)
    ze = lax.broadcasted_iota(jnp.int32, (2 * LANES, 1), 0)
    zf = ze.astype(F32)
    cells_z = jnp.where(ze < bz + HALO, zf + HALO, jnp.where(ze < bz + 2 * HALO, zf - (bz + HALO), FAR))
    sub_x = lax.broadcasted_iota(jnp.int32, (LANES, LANES), 0).astype(F32)
    lane_x = lax.broadcasted_iota(jnp.int32, (2 * LANES, LANES), 1).astype(F32)
    dot = lambda a, b: jnp.dot(a, b, preferred_element_type=F32)

    def matrices(j, source):
        rx, ry, rz = source[0:1, :], source[1:2, :], source[2:3, :]
        xm = wrapped(rx + HALO, total_x)
        ys = wrapped(ry - fiy * by, total_y)
        zs = wrapped(rz + HALO - fiz * bz, total_z)
        for p in range(3):
            target = wrapped(fspot[0] + (1 - p), n) * bx
            hit = jnp.logical_and(lane_r < slots, jnp.logical_and(xm >= target, xm < target + bx))
            some = lane_sum(jnp.where(hit, 1.0, 0.0)) > 0.5
            sx = lane_sum(jnp.where(hit, xm, 0.0)) - target
            sy = lane_sum(jnp.where(hit, ys, 0.0))
            sz = lane_sum(jnp.where(hit, zs, 0.0))
            place = jnp.where(some, cells_y - sy, FAR)
            place = jnp.where(jnp.logical_and(place < 0, place > FAR / 2), place + total_y, place)
            hot = jnp.where(sub_x == place, 1.0, 0.0).astype(BF)
            m = dot(tab[...], hot).astype(BF)
            lhs[p, bank[j] * G:(bank[j] + 1) * G, :half] = m[:G]
            lhs[p, bank[j] * G:(bank[j] + 1) * G, half:2 * half] = m[:G]
            lhs[p, bank[j] * G:(bank[j] + 1) * G, 2 * half:] = m[G:]
            place = jnp.where(some, cells_z - sz, FAR)
            hot = jnp.where(lane_x == place, 1.0, 0.0).astype(BF)
            wz[j, p] = dot(hot, tabt[...]).astype(BF)
            if p == 1:
                place = jnp.where(some, cols[4:5, :LANES] - sx, FAR)
                hot = jnp.where(sub_x == place, 1.0, 0.0).astype(BF)
                m = dot(tab[...], hot).astype(BF)
                ma[j, :, :LANES] = m[:G]
                ma[j, :, LANES:] = m[G:]

    for j in range(n):
        outb[j, SIDES + 8 + G:] = jnp.zeros((BLOCK - SIDES - 8 - G, G * G), F32)
        if j:
            got[j, SIDES + 8 + G:] = jnp.zeros((BLOCK - SIDES - 8 - G, G * G), F32)
    matrices(0, rt.at[0])
    xm = wrapped(rt[0, 0:1, :] + HALO, total_x)
    hots = []
    wide = cols.shape[1]
    sub_w = lax.broadcasted_iota(jnp.int32, (LANES, wide), 0).astype(F32)
    ext, shifted, turn, inner = cols[0:1, :], cols[1:2, :], cols[2:3, :], cols[3:4, :]
    srcs = jnp.zeros((1, wide), F32)
    for j in range(n):
        srcs = jnp.where(turn == j, fspot[j], srcs)
    high_rows = G * slots
    line = lax.broadcasted_iota(jnp.int32, (high_rows, 1), 0)
    line_f = lax.rem(line, slots)
    line_a = (line - line_f).astype(F32) * (1.0 / slots)
    slab_of = jnp.zeros((high_rows, 1), F32)
    for f in range(slots):
        mine = lane_sum(jnp.where(lane_r == f, xm, 0.0))
        slab = jnp.zeros((1, 1), F32)
        for k in range(1, n):
            slab = slab + jnp.where(mine >= k * bx, 1.0, 0.0)
        t = shifted + (slab - srcs)
        good = jnp.logical_or(t == 0, jnp.logical_or(t == n, t == -n))
        place = jnp.where(good, ext - (mine - slab * bx), FAR)
        hots.append(jnp.where(sub_w == place, 1.0, 0.0).astype(BF))
        slab_of = jnp.where(line_f == f, slab, slab_of)
    m = dot(tabi[...], jnp.concatenate(hots, axis=0))
    same = jnp.logical_and(line_a == inner, slab_of == srcs)
    mx[:high_rows] = jnp.where(same, 1.0, m[:high_rows]).astype(BF)
    mx[high_rows:] = m[high_rows:].astype(BF)
    for j in range(1, n):
        root_copy[j].wait_recv()
        matrices(j, rt.at[j])

    lane_h = lax.broadcasted_iota(jnp.int32, (pad, LANES), 1)
    blank = jnp.zeros((pad - by, LANES), F32)

    def full(v):
        return jnp.concatenate([v, blank], axis=0)

    def keep(x, c, side, v):
        h, l = split(v)
        lanes = slice(side * LANES, (side + 1) * LANES)
        yb[x, c * pad:(c + 1) * pad, lanes] = h
        yb[x, half + c * pad:half + (c + 1) * pad, lanes] = l

    def inner_row(c, block):
        def one(x, carry):
            keep(x, c, 0, full(block[x]))
            return carry
        return one

    def halo_row(x, carry):
        t = HALO * x // LANES
        at = HALO * x - LANES * t
        t_next = (HALO * x + HALO - 1) // LANES
        back = lax.rem(LANES - at, LANES)
        for c, halos in enumerate((zin, zpeer)):
            def piece(side, place):
                turn = lax.rem(back + place, LANES)
                one = pltpu.roll(full(halos[side, t]), turn, 1)
                two = pltpu.roll(full(halos[side, t_next]), turn, 1)
                return jnp.where(lane_h - place < LANES - at, one, two)
            second = jnp.where(lane_h < HALO, piece(1, 0), jnp.where(lane_h < 2 * HALO, piece(0, HALO), 0.0))
            keep(x, c, 1, second)
        return carry

    def row(p, x, s, group):
        first, count = (bank[0] * G, G) if group == [0] else (0, (n - 1) * G)
        m = slice(first, first + count)
        r = dot(lhs[p, m, :2 * half], yb[x]) + dot(lhs[p, m, 2 * half:], yb[x, :half])
        for side in range(2):
            us[side, pl.ds(first * 8 + s, count, stride=8), :] = r[:, side * LANES:(side + 1) * LANES]

    def finish(j, p):
        held = slice(bank[j] * G * 8, (bank[j] + 1) * G * 8)
        h, l = split(jnp.concatenate([us[0, held], us[1, held]], axis=1))
        a = dot(h, wz[j, p])
        return a[:, :LANES] + a[:, LANES:] + dot(l, wz[j, p, :, :LANES])

    def store(ref, j, at, r):
        for b in range(G):
            ref[j, pl.ds(at, 8), b * G:(b + 1) * G] = r[8 * b:8 * b + 8, :G]

    def sent(j, q):
        at = pl.ds(pl.multiple_of(8 * q, 8), 8)
        return copy(outb.at[j, at], got.at[j, at], gx_s.at[j, q], gx_r.at[j, q], other[j])

    def sent_mid(j):
        at = pl.ds(SIDES + 8, G)
        q = SIDES // 8 + 1
        return copy(outb.at[j, at], got.at[j, at], gx_s.at[j, q], gx_r.at[j, q], other[j])

    def emit(work, send, group):
        previous = None
        for j in group:
            work(j)
            if previous:
                send(previous).start()
            previous = j

    def side_octet(group, c0):
        def one(c, carry):
            p, x0 = octet_place(bx, 2 * c)
            for s in range(8):
                row(p, x0 + s, s, group)
            if group[-1]:
                @pl.when(c > c0)
                def _():
                    sent(group[-1], c - 1).start()
            emit(lambda j: store(outb, j, pl.multiple_of(8 * c, 8), finish(j, p)), lambda j: sent(j, c), group)
            return carry
        return one

    def mid_octet(group):
        def one(c, carry):
            for s in range(8):
                row(1, 8 * c + s, s, group)
            for j in group:
                store(mids, j, pl.multiple_of(8 * c, 8), finish(j, 1))
            return carry
        return one

    def tail_octet(group):
        for k, (p, x) in enumerate(tail):
            row(p, x, k, group)
        if group[-1]:
            sent(group[-1], SIDES // 8 - 1).start()
        sub = lax.broadcasted_iota(jnp.int32, (G * 8, LANES), 0) % 8

        def work(j):
            total = jnp.zeros((G * 8, LANES), F32)
            for p in range(3):
                places = [k for k, t in enumerate(tail) if t[0] == p]
                mine = jnp.logical_and(sub >= places[0], sub <= places[-1])
                total = jnp.where(mine, finish(j, p), total)
            store(outb, j, SIDES, total)
            store(mids, j, MIDS - 8, total)

        emit(work, lambda j: sent(j, SIDES // 8), group)

    lax.fori_loop(0, bx, inner_row(0, pot), 0)
    for c in raw:
        c.wait_recv()
    lax.fori_loop(0, bx, inner_row(1, peer), 0)
    for c in zc[0]:
        c.wait_recv()
    for c in rel[0]:
        c.start()
    for s, (x0, x1, i0, i1, _, _) in enumerate(plan):
        for c in rel[s]:
            c.wait_recv()
        lax.fori_loop(x0, x1, halo_row, 0)
        c0, c1 = (i0 + 1) // 2, (i1 + 1) // 2
        lax.fori_loop(c0, c1, side_octet(order, c0), 0)
        if s < last:
            for c in zc[s + 1]:
                c.wait_recv()
            for c in rel[s + 1]:
                c.start()
            if c1 > c0:
                sent(order[-1], c1 - 1).start()
        else:
            tail_octet(order)
        lax.fori_loop(i0 // 2, i1 // 2, mid_octet(order), 0)

    tile = 2 * LANES
    tiles = G * G // tile

    def mid_work(j):
        def one(t, carry):
            at = pl.ds(pl.multiple_of(t * tile, tile), tile)
            h, l = split(mids[j, :, at])
            both = jnp.concatenate([h, l], axis=0)
            outb[j, SIDES + 8:SIDES + 8 + G, at] = (
                dot(ma[j, :, :2 * MIDS], both) + dot(ma[j, :, LANES:LANES + MIDS], h))
            return carry
        lax.fori_loop(0, tiles, one, 0)

    sent(order[-1], SIDES // 8).start()
    emit(mid_work, sent_mid, order)
    for s in range(8):
        row(2, s, s, [0])
    sent_mid(order[-1]).start()
    lax.fori_loop(0, SIDES // 8, side_octet([0], 0), 0)
    lax.fori_loop(0, octets // 2, mid_octet([0]), 0)
    tail_octet([0])
    mid_work(0)

    def gather_rows(first, rows, at):
        return jnp.concatenate([outb[0, first:first + rows, at]] + [got[j, first:first + rows, at]
                                                                    for j in range(1, n)], axis=0)

    def across(first, rows, k0, at):
        h, l = split(gather_rows(first, rows, at))
        both = dot(mx[:, k0:k0 + n * 64], h)
        return both[:high_rows] + both[high_rows:] + dot(mx[:high_rows, k0:k0 + n * 64], l)

    for s in range(last + 1):
        raw[s].wait_send()
        for c in zc[s] + rel[s]:
            c.wait_send()
    for j in range(1, n):
        root_copy[j].wait_send()

    def arrived(q, carry):
        for j in range(1, n):
            sent(j, q).wait()
        return carry

    lax.fori_loop(0, SIDES // 8, arrived, 0)

    def first_part(t, carry):
        at = pl.ds(pl.multiple_of(t * tile, tile), tile)
        acc[:, at] = across(0, SIDES, 0, at)
        return carry

    lax.fori_loop(0, tiles, first_part, 0)
    arrived(SIDES // 8, 0)
    for j in range(1, n):
        sent_mid(j).wait()

    def second_part(t, carry):
        at = pl.ds(pl.multiple_of(t * tile, tile), tile)
        r = acc[:, at] + across(SIDES, 64, n * 64, at)
        for a in range(G):
            where = pl.multiple_of(a * G * G + t * tile, LANES)
            out[:, pl.ds(where, tile)] = r[a * slots:(a + 1) * slots]
        return carry

    lax.fori_loop(0, tiles, second_part, 0)


def fused(info, pot, roots, consts):
    n, ny, nz, slots = info
    bx, by, bz = pot.shape
    octets = layout(bx)[3]
    chunks = len(CHUNKS)
    pad = -(-by // 16) * 16
    half = ny * pad
    dma = pltpu.SemaphoreType.DMA
    vmem = pl.BlockSpec(memory_space=pltpu.VMEM)
    folded = (2, tiles_of(bx), by, LANES)
    return pl.pallas_call(
        lambda *refs: fused_kernel(info, *refs),
        in_specs=[pl.BlockSpec(memory_space=pl.ANY)] + [vmem] * 5,
        out_specs=vmem,
        out_shape=jax.ShapeDtypeStruct((slots, G ** 3), F32),
        scratch_shapes=[
            pltpu.VMEM((bx, by, LANES), F32),
            pltpu.VMEM((n, BLOCK, G * G), F32),
            pltpu.VMEM((2 * G * slots, 2 * n * 64), BF),
            pltpu.VMEM((bx, by, LANES), F32),
            pltpu.VMEM(folded, F32),
            pltpu.VMEM(folded, F32),
            pltpu.VMEM(folded, F32),
            pltpu.VMEM((n, 8, LANES), F32),
            pltpu.VMEM((bx, 2 * half, 2 * LANES), BF),
            pltpu.VMEM((3, n * G, 3 * half), BF),
            pltpu.VMEM((n, 3, 2 * LANES, 2 * LANES), BF),
            pltpu.VMEM((2, n * G * 8, LANES), F32),
            pltpu.VMEM((n, BLOCK, G * G), F32),
            pltpu.VMEM((n, MIDS, G * G), F32),
            pltpu.VMEM((n, G, 2 * LANES), BF),
            pltpu.VMEM((G * slots, G * G), F32),
            dma, dma((chunks,)), dma((chunks,)),
            dma((2, chunks)), dma((2, chunks)),
            dma((2, chunks)), dma((2, chunks)),
            dma((n,)), dma((n,)),
            dma((n, SIDES // 8 + 2)), dma((n, SIDES // 8 + 2)),
        ],
        compiler_params=pltpu.CompilerParams(
            collective_id=0, has_side_effects=True, vmem_limit_bytes=56 * 1024 * 1024),
        cost_estimate=pl.CostEstimate(flops=24 * 10 ** 9, bytes_accessed=16 * 1024 * 1024, transcendentals=0),
        name="exchange_contract",
    )(pot, roots, *consts)


def body(potential, frag_root):
    bx, by, bz = potential.shape
    n, ny, nz = lax.axis_size("gx"), lax.axis_size("gy"), lax.axis_size("gz")
    slots = frag_root.shape[1]
    if n != 4:
        return plain_body(potential, frag_root)
    consts = [jnp.asarray(c) for c in tables(bx, n, slots)]
    return fused((n, ny, nz, slots), potential, frag_root, consts)


def solution(mesh):
    return jax.shard_map(
        body,
        mesh=mesh,
        in_specs=(P("gx", "gy", "gz"), P(None, ("gx", "gy", "gz"))),
        out_specs=P(("gx", "gy", "gz"), None),
        check_vma=False,
    )
```

```python
import math

import jax
import jax.numpy as jnp
import numpy as np
from jax import lax
from jax.experimental import pallas as pl
from jax.experimental.pallas import tpu as pltpu
from jax.sharding import PartitionSpec as P

G = 48
BOX = 68
HALO = 34
LANES = 128
FOLD = LANES // HALO
BF = jnp.bfloat16
F32 = jnp.float32
MESH = pl.DeviceIdType.MESH
FAR = -1.0e6
FAR_CELL = -(1 << 20)
STEPS = 4
HIGH = lax.Precision.HIGH


def interp_values():
    offset = np.arange(G)[:, None] * BOX - np.arange(BOX)[None, :] * G
    summed = np.ones((G, BOX))
    for harmonic in range(1, G // 2):
        summed += 2.0 * np.cos(2.0 * math.pi / (G * BOX) * np.mod(harmonic * offset, G * BOX))
    return (summed / BOX).astype(np.float32)


def halves(value):
    high = value.astype(BF)
    return high, (value - high.astype(np.float32)).astype(BF)


def split(value):
    high = value.astype(BF)
    return high, (value - high.astype(F32)).astype(BF)


def shift(array, axis, step):
    devices = lax.axis_size(axis)
    return lax.ppermute(array, axis, [(i, (i + step) % devices) for i in range(devices)])


def placed(start, cells, period, valid):
    place = cells - start[..., None]
    if period:
        place = jnp.mod(place, period)
    inside = jnp.logical_and(place >= 0, place < BOX)
    inside = jnp.logical_and(inside, valid[..., None])
    base = jnp.asarray(interp_values())
    index = jnp.where(inside, place, BOX)
    hot = (index[..., None, :] == jnp.arange(BOX, dtype=jnp.int32)[:, None]).astype(jnp.float32)
    return jnp.einsum("ax,...xe->...ae", base, hot, precision=lax.Precision.HIGHEST)


def pack_kernel(pot, low, high):
    rows, by = pot.shape[1], pot.shape[2]
    lane = lax.broadcasted_iota(jnp.int32, (rows * by, LANES), 1)
    down = jnp.zeros((rows * by, LANES), F32)
    up = down
    for g in range(FOLD):
        v = pot[g].reshape(rows * by, LANES)
        mine = jnp.logical_and(lane >= g * HALO, lane < (g + 1) * HALO)
        down = jnp.where(mine, pltpu.roll(v, ((g + 1) * HALO) % LANES, 1), down)
        up = jnp.where(mine, pltpu.roll(v, g * HALO, 1) if g else v, up)
    low[...] = down.reshape(rows, by, LANES)
    high[...] = up.reshape(rows, by, LANES)


def pack(pot):
    fold, rows, by, bz = pot.shape
    step = rows // STEPS
    spec = pl.BlockSpec((step, by, LANES), lambda i: (i, 0, 0))
    shape = jax.ShapeDtypeStruct((rows, by, LANES), F32)
    return pl.pallas_call(
        pack_kernel,
        grid=(STEPS,),
        in_specs=[pl.BlockSpec((fold, step, by, LANES), lambda i: (0, i, 0, 0))],
        out_specs=[spec, spec],
        out_shape=[shape, shape],
        cost_estimate=pl.CostEstimate(flops=0, bytes_accessed=4 * pot.size * 2, transcendentals=0),
        name="pack_halos",
    )(pot)


def plain_slab_kernel(ny, *refs):
    owns, lows, highs, out = refs[:ny], refs[ny:2 * ny], refs[2 * ny:3 * ny], refs[3 * ny]
    rows, by = owns[0].shape[1], owns[0].shape[2]
    pad = out.shape[2] // (2 * ny)
    half = ny * pad
    lane = lax.broadcasted_iota(jnp.int32, (pad, LANES), 1)
    blank = jnp.zeros((pad - by, LANES), F32)

    def full(v):
        return jnp.concatenate([v, blank], axis=0)

    for c in range(ny):
        for r in range(rows):
            up = full(highs[c][r])
            down = full(lows[c][r])
            for g in range(FOLD):
                first = full(owns[c][g, r])
                a = pltpu.roll(up, (-g * HALO) % LANES, 1) if g else up
                b = pltpu.roll(down, (HALO - g * HALO) % LANES, 1) if g != 1 else down
                second = jnp.where(lane < HALO, a, jnp.where(lane < 2 * HALO, b, 0.0))
                for side, v in ((0, first), (1, second)):
                    h, l = split(v)
                    cols = slice(side * LANES, (side + 1) * LANES)
                    out[g, r, c * pad:(c + 1) * pad, cols] = h
                    out[g, r, half + c * pad:half + (c + 1) * pad, cols] = l


def slabs(owns, lows, highs):
    ny = len(owns)
    fold, rows, by, bz = owns[0].shape
    pad = -(-by // 16) * 16
    step = rows // STEPS
    big = pl.BlockSpec((fold, step, by, LANES), lambda i: (0, i, 0, 0))
    small = pl.BlockSpec((step, by, LANES), lambda i: (i, 0, 0))
    return pl.pallas_call(
        lambda *refs: plain_slab_kernel(ny, *refs),
        grid=(STEPS,),
        in_specs=[big] * ny + [small] * (2 * ny),
        out_specs=pl.BlockSpec((fold, step, 2 * ny * pad, 2 * LANES), lambda i: (0, i, 0, 0)),
        out_shape=jax.ShapeDtypeStruct((fold, rows, 2 * ny * pad, 2 * LANES), BF),
        cost_estimate=pl.CostEstimate(flops=0, bytes_accessed=16 * 1024 * 1024, transcendentals=0),
        name="build_slabs",
    )(*owns, *lows, *highs)


def contract_kernel(bx, yb, my, mz, out, lhs, wz, us):
    k = my.shape[2]
    for p in range(3):
        h, l = split(my[p])
        lhs[p, :G, :k] = h
        lhs[p, :G, k:] = h
        lhs[p, G:, :k] = l
        lhs[p, G:, k:] = jnp.zeros_like(l)
        h, l = split(mz[p])
        wz[p, 0] = h
        wz[p, 1] = l
    nl, nm = HALO // 8, bx // 8

    def row(p, x, s):
        r = jnp.dot(lhs[p], yb[x], preferred_element_type=F32)
        us[:, s, :] = r[:G] + r[G:]

    def finish(p):
        h, l = split(us[...].reshape(G * 8, us.shape[2]))
        dot = lambda a, b: jnp.dot(a, b, preferred_element_type=F32)
        return dot(h, wz[p, 0]) + dot(h, wz[p, 1]) + dot(l, wz[p, 0])

    def store(r, row0):
        for b in range(G):
            out[pl.ds(row0, 8), b * G:(b + 1) * G] = r[8 * b:8 * b + 8]

    def block(i, carry):
        p = (i >= nl).astype(jnp.int32) + (i >= nl + nm).astype(jnp.int32)
        x0 = jnp.where(p == 0, bx - HALO + 8 * i, jnp.where(p == 1, 8 * (i - nl), 8 * (i - nl - nm)))
        for s in range(8):
            row(p, x0 + s, s)
        store(finish(p), pl.multiple_of(8 * i, 8))
        return carry

    blocks = 2 * nl + nm
    lax.fori_loop(0, blocks, block, 0)
    tail = plain_tail_rows(bx)
    for s, (p, x) in enumerate(tail):
        row(p, x, s)
    sub = lax.broadcasted_iota(jnp.int32, (G * 8, G), 0) % 8
    total = jnp.zeros((G * 8, G), F32)
    for p in range(3):
        places = [s for s, t in enumerate(tail) if t[0] == p]
        mine = jnp.logical_and(sub >= places[0], sub <= places[-1])
        total = jnp.where(mine, finish(p), total)
    store(total, 8 * blocks)


def plain_tail_rows(bx):
    nl, nm = HALO // 8 * 8, bx // 8 * 8
    rows = [(0, bx - HALO + x) for x in range(nl, HALO)]
    rows += [(1, x) for x in range(nm, bx)]
    rows += [(2, x) for x in range(nl, HALO)]
    assert len(rows) == 8
    return rows


def plain_row_order(bx):
    nl, nm = HALO // 8 * 8, bx // 8 * 8
    rows = [(0, bx - HALO + x) for x in range(nl)] + [(1, x) for x in range(nm)]
    return rows + [(2, x) for x in range(nl)] + plain_tail_rows(bx)


def contract(bx, yb, my, mz):
    rows = len(plain_row_order(bx))
    k = my.shape[2]
    width = yb.shape[2]
    return pl.pallas_call(
        lambda *refs: contract_kernel(bx, *refs),
        in_specs=[pl.BlockSpec(memory_space=pltpu.VMEM)] * 3,
        out_specs=pl.BlockSpec(memory_space=pltpu.VMEM),
        out_shape=jax.ShapeDtypeStruct((rows, G * G), F32),
        scratch_shapes=[
            pltpu.VMEM((3, 2 * G, 2 * k), BF),
            pltpu.VMEM((3, 2, width, G), BF),
            pltpu.VMEM((G, 8, width), F32),
        ],
        compiler_params=pltpu.CompilerParams(vmem_limit_bytes=40 * 1024 * 1024),
        cost_estimate=pl.CostEstimate(
            flops=6 * 10 ** 9, bytes_accessed=2 * yb.size + 4 * rows * G * G, transcendentals=0),
        name="contract_yz",
    )(yb, my, mz)


def plain_body(potential, frag_root):
    bx, by, bz = potential.shape
    n = lax.axis_size("gx")
    ny = lax.axis_size("gy")
    nz = lax.axis_size("gz")
    ix, iy, iz = lax.axis_index("gx"), lax.axis_index("gy"), lax.axis_index("gz")
    total_x, total_y, total_z = bx * n, by * ny, bz * nz
    slots = frag_root.shape[1]

    folded = potential.reshape(FOLD, bx // FOLD, by, bz)
    low, high = pack(folded)
    low = shift(low, "gz", 1)
    high = shift(high, "gz", -1)
    owns = [folded] + [shift(folded, "gy", -j) for j in range(1, ny)]
    lows = [low] + [shift(low, "gy", -j) for j in range(1, ny)]
    highs = [high] + [shift(high, "gy", -j) for j in range(1, ny)]
    root = jnp.stack([frag_root] + [shift(frag_root, "gx", j) for j in range(1, n)])
    yb = slabs(owns, lows, highs)
    yb = yb.reshape(bx, yb.shape[2], yb.shape[3])

    anchor = jnp.mod(root[:, 0] + HALO, total_x) // bx
    start_y = jnp.mod(root[:, 1] - iy * by, total_y)
    start_z = jnp.mod(root[:, 2] + HALO - iz * bz, total_z)
    pad = -(-by // 16) * 16
    e = jnp.arange(ny * pad, dtype=jnp.int32)
    cells_y = e // pad * by + e % pad
    real_y = e % pad < by
    e = jnp.arange(2 * LANES, dtype=jnp.int32)
    cells_z = jnp.where(e < bz + HALO, e + HALO, jnp.where(e < bz + 2 * HALO, e - bz - HALO, FAR_CELL))
    delta = jnp.array([1, 0, -1], jnp.int32)
    hit = anchor[:, None, :] == jnp.mod(ix + delta, n)[None, :, None]
    valid = jnp.any(hit, axis=2)
    pick = lambda v: jnp.sum(jnp.where(hit, v[:, None, :], 0), axis=2)
    my = placed(pick(start_y), cells_y, total_y, valid)
    my = jnp.where(real_y, my, 0.0)
    mz = placed(pick(start_z), cells_z, None, valid).transpose(0, 1, 3, 2)

    order = [j for j in range(2, n, 2)] + [j for j in range(n) if j % 2]
    got = [None] * n
    for j in order:
        got[j] = shift(contract(bx, yb, my[j], mz[j]), "gx", -j)
    got[0] = contract(bx, yb, my[0], mz[0])

    mine = jnp.mod(frag_root[0] + HALO, total_x)
    slab = mine // bx
    rel = mine - slab * bx
    rows = plain_row_order(bx)
    part = jnp.array([p for p, x in rows], jnp.int32)
    ext = jnp.array([x - (bx - HALO) if p == 0 else x + HALO + (p - 1) * bx for p, x in rows], jnp.int32)
    mx = placed(rel, ext, None, jnp.ones((slots,), bool))
    source = jnp.mod(slab[:, None] - ix + part[None, :] - 1, n)
    fields = None
    for j in [0] + order:
        m = jnp.where((source == j)[:, None, :], mx, 0.0).reshape(slots * G, -1)
        term = jnp.dot(m, got[j], precision=HIGH)
        fields = term if fields is None else fields + term
    return fields.reshape(slots, -1)


def octet_place(bx, i):
    c = i // 2
    odd = i % 2 == 1
    first = i < 2 * (HALO // 8)
    if isinstance(i, int):
        return (1, 8 * c) if odd else ((2, 8 * c) if first else (0, bx - HALO + 8 * (c - HALO // 8)))
    p = jnp.where(odd, 1, jnp.where(first, 2, 0))
    x0 = jnp.where(jnp.logical_or(odd, first), 8 * c, bx - HALO + 8 * (c - HALO // 8))
    return p, x0


def layout(bx):
    octets = bx // 8 + 2 * (HALO // 8)
    placed_rows = [(p, x0 + s) for p, x0 in (octet_place(bx, i) for i in range(octets)) for s in range(8)]
    tail = [(0, x) for x in range(bx - HALO, bx)] + [(1, x) for x in range(bx)] + [(2, x) for x in range(HALO)]
    tail = [t for t in tail if t not in placed_rows]
    assert len(tail) == 8 and len(set(placed_rows + tail)) == len(placed_rows) + 8
    sides = [t for i in range(0, octets + 1, 2) for t in placed_rows[8 * i:8 * i + 8] if t[0] != 1]
    mids = [t for t in placed_rows if t[0] == 1]
    assert len(sides) == SIDES and len(mids) + 8 == MIDS
    return sides, mids, tail, octets


SIDES = 2 * (HALO // 8) * 8
MIDS = 64
BLOCK = SIDES + 64
CHUNKS = (3, 2, 2, 3, 2, 2, 2)


def tables(bx, n, slots):
    high, low = halves(interp_values())
    tab = np.zeros((2 * G, LANES), BF)
    tab[:G, :BOX], tab[G:, :BOX] = high, low
    tabt = np.zeros((LANES, 2 * LANES), BF)
    tabt[:BOX, :G], tabt[:BOX, LANES:LANES + G] = high.T, low.T
    tabi = np.zeros((2, G, slots, slots, LANES), BF)
    for f in range(slots):
        tabi[0, :, f, f, :BOX], tabi[1, :, f, f, :BOX] = high, low
    tabi = tabi.reshape(2 * G * slots, slots * LANES)
    sides, mids, tail, _ = layout(bx)
    reach = lambda p, x: x - (bx - HALO) + (0, bx, 2 * bx)[p]
    cols = np.full((8, 2 * n * 64), FAR, np.float32)
    for j in range(n):
        for half, rows in ((0, sides), (1, [t if t[0] != 1 else None for t in tail])):
            for r, t in enumerate(rows):
                if t:
                    cols[0:2, half * n * 64 + j * 64 + r] = reach(*t), t[0] - 1
        for half in (0, 1):
            cols[2, half * n * 64 + j * 64:half * n * 64 + (j + 1) * 64] = j
        for a in range(G):
            cols[3, n * 64 + j * 64 + 8 + a] = a
    for r, t in enumerate(mids + tail):
        if t[0] == 1:
            cols[4, r] = cols[4, MIDS + r] = reach(*t)
    return tab, tabt, tabi, cols


def stages(bx, octets):
    need = [octet_place(bx, i)[1] + 8 for i in range(octets)]
    plan, i, t = [], 0, 0
    for count in CHUNKS:
        start, end = i, t + count
        x0, x1 = min(t * LANES // HALO, bx), min(end * LANES // HALO, bx)
        while i < octets and need[i] <= x1:
            i += 1
        plan.append((x0, x1, start, i, t, end))
        t = end
    assert x1 == bx and t == tiles_of(bx) and i == octets
    return plan


def tiles_of(bx):
    return -(-bx * HALO // LANES)


def fused_kernel(info, pot_hbm, own_root, tab, tabt, tabi, cols, out, pot, got, mx, peer, pack, zin, zpeer, rt, yb,
                 lhs, wz, us, outb, mids, ma, acc, load_s, raw_s, raw_r, z_s, z_r, rel_s, rel_r, rt_s, rt_r,
                 gx_s, gx_r):
    n, ny, nz, slots = info
    bx, by, bz = pot.shape
    total_x, total_y, total_z = bx * n, by * ny, bz * nz
    side_rows, mid_rows, tail, octets = layout(bx)
    plan = stages(bx, octets)
    last = len(plan) - 1
    pad = yb.shape[1] // (2 * ny)
    half = ny * pad
    ix, iy, iz = lax.axis_index("gx"), lax.axis_index("gy"), lax.axis_index("gz")
    mate = {"gy": lax.rem(iy + 1, ny)}
    above = {"gz": lax.rem(iz + 1, nz)}
    below = {"gz": lax.rem(iz + nz - 1, nz)}
    spot = [ix, ix + 1 - 2 * lax.rem(ix, 2), lax.rem(ix + 2, 4), 3 - ix]
    other = [{"gx": d} for d in spot]
    order = [3, 1, 2]
    bank = [3, 0, 1, 2]

    def copy(src, dst, ss, rs, where):
        return pltpu.make_async_remote_copy(
            src_ref=src, dst_ref=dst, send_sem=ss, recv_sem=rs, device_id=where, device_id_type=MESH)

    lead = plan[0][1] + 1
    loads = [pltpu.make_async_copy(pot_hbm.at[rows], pot.at[rows], load_s.at[k])
             for k, rows in enumerate((slice(0, lead), slice(lead, bx)))]
    for load in loads:
        load.start()
    barrier = pltpu.get_barrier_semaphore()
    friends = [above, below, mate] + other[1:]
    for where in friends:
        pl.semaphore_signal(barrier, inc=1, device_id=where, device_id_type=MESH)

    root_copy = [None] + [copy(rt.at[0], rt.at[j], rt_s.at[j], rt_r.at[j], other[j]) for j in range(1, n)]
    raw, zc, rel = [], [], []
    for s, (x0, x1, _, _, t0, t1) in enumerate(plan):
        xs = slice(x0, x1)
        rs = slice(t0, t1)
        raw.append(copy(pot.at[xs], peer.at[xs], raw_s.at[s], raw_r.at[s], mate))
        zc.append([copy(pack.at[side, rs], zin.at[side, rs], z_s.at[side, s], z_r.at[side, s], where)
                   for side, where in ((0, above), (1, below))])
        rel.append([copy(zin.at[side, rs], zpeer.at[side, rs], rel_s.at[side, s], rel_r.at[side, s], mate)
                    for side in (0, 1)])

    lane_p = lax.broadcasted_iota(jnp.int32, (by, LANES), 1)

    def pack_tile(t, limit):
        down = jnp.zeros((by, LANES), F32)
        up = down
        x0 = LANES * t // HALO
        for k in range(-(-LANES // HALO) + 1):
            x = jnp.minimum(x0 + k, limit - 1)
            at = HALO * x - LANES * t
            v = pot[x]
            mine = jnp.logical_and(lane_p >= at, lane_p < at + HALO)
            down = jnp.where(mine, pltpu.roll(v, lax.rem(at + HALO + LANES, LANES), 1), down)
            up = jnp.where(mine, pltpu.roll(v, lax.rem(at + LANES, LANES), 1), up)
        pack[0, t] = down
        pack[1, t] = up

    def pack_tiles(t0, t1, limit):
        lax.fori_loop(t0, t1, lambda t, carry: (pack_tile(t, limit), carry)[1], 0)

    rt[0] = jnp.zeros(rt.shape[1:], F32)
    rt[0, :3, :slots] = own_root[...].astype(F32)
    loads[0].wait()
    pack_tiles(*plan[0][4:], lead)
    loads[1].wait()
    pl.semaphore_wait(barrier, len(friends))
    for s in range(last + 1):
        if 0 < s < last:
            pack_tiles(*plan[s + 1][4:], bx)
        for c in zc[s]:
            c.start()
        raw[s].start()
        if s == 0:
            for j in range(1, n):
                root_copy[j].start()
            pack_tiles(*plan[1][4:], bx)
        if s == last - 1:
            for j in range(n):
                outb[j, SIDES + 8 + G:] = jnp.zeros((BLOCK - SIDES - 8 - G, G * G), F32)
                if j:
                    got[j, SIDES + 8 + G:] = jnp.zeros((BLOCK - SIDES - 8 - G, G * G), F32)

    lane_r = lax.broadcasted_iota(jnp.int32, (1, LANES), 1)
    fiy, fiz = iy.astype(F32), iz.astype(F32)
    fspot = [d.astype(F32) for d in spot]

    def wrapped(v, period):
        v = jnp.where(v < 0, v + period, v)
        return jnp.where(v >= period, v - period, v)

    def lane_sum(v):
        return jnp.sum(v, axis=1, keepdims=True)

    ye = lax.broadcasted_iota(jnp.int32, (1, half), 1)
    block_y = jnp.zeros((1, half), jnp.int32)
    for c in range(1, ny):
        block_y = block_y + (ye >= c * pad).astype(jnp.int32)
    real_y = ye - block_y * pad < by
    cells_y = jnp.where(real_y, (ye - block_y * (pad - by)).astype(F32), FAR)
    ze = lax.broadcasted_iota(jnp.int32, (2 * LANES, 1), 0)
    zf = ze.astype(F32)
    cells_z = jnp.where(ze < bz + HALO, zf + HALO, jnp.where(ze < bz + 2 * HALO, zf - (bz + HALO), FAR))
    sub_x = lax.broadcasted_iota(jnp.int32, (LANES, LANES), 0).astype(F32)
    lane_x = lax.broadcasted_iota(jnp.int32, (2 * LANES, LANES), 1).astype(F32)
    dot = lambda a, b: jnp.dot(a, b, preferred_element_type=F32)

    def matrices(j, source):
        rx, ry, rz = source[0:1, :], source[1:2, :], source[2:3, :]
        xm = wrapped(rx + HALO, total_x)
        ys = wrapped(ry - fiy * by, total_y)
        zs = wrapped(rz + HALO - fiz * bz, total_z)
        for p in range(3):
            target = wrapped(fspot[0] + (1 - p), n) * bx
            hit = jnp.logical_and(lane_r < slots, jnp.logical_and(xm >= target, xm < target + bx))
            some = lane_sum(jnp.where(hit, 1.0, 0.0)) > 0.5
            sx = lane_sum(jnp.where(hit, xm, 0.0)) - target
            sy = lane_sum(jnp.where(hit, ys, 0.0))
            sz = lane_sum(jnp.where(hit, zs, 0.0))
            place = jnp.where(some, cells_y - sy, FAR)
            place = jnp.where(jnp.logical_and(place < 0, place > FAR / 2), place + total_y, place)
            hot = jnp.where(sub_x == place, 1.0, 0.0).astype(BF)
            m = dot(tab[...], hot).astype(BF)
            lhs[p, bank[j] * G:(bank[j] + 1) * G, :half] = m[:G]
            lhs[p, bank[j] * G:(bank[j] + 1) * G, half:2 * half] = m[:G]
            lhs[p, bank[j] * G:(bank[j] + 1) * G, 2 * half:] = m[G:]
            place = jnp.where(some, cells_z - sz, FAR)
            hot = jnp.where(lane_x == place, 1.0, 0.0).astype(BF)
            wz[j, p] = dot(hot, tabt[...]).astype(BF)
            if p == 1:
                place = jnp.where(some, cols[4:5, :LANES] - sx, FAR)
                hot = jnp.where(sub_x == place, 1.0, 0.0).astype(BF)
                m = dot(tab[...], hot).astype(BF)
                ma[j, :, :LANES] = m[:G]
                ma[j, :, LANES:] = m[G:]

    matrices(0, rt.at[0])
    xm = wrapped(rt[0, 0:1, :] + HALO, total_x)
    hots = []
    wide = cols.shape[1]
    sub_w = lax.broadcasted_iota(jnp.int32, (LANES, wide), 0).astype(F32)
    ext, shifted, turn, inner = cols[0:1, :], cols[1:2, :], cols[2:3, :], cols[3:4, :]
    srcs = jnp.zeros((1, wide), F32)
    for j in range(n):
        srcs = jnp.where(turn == j, fspot[j], srcs)
    high_rows = G * slots
    line = lax.broadcasted_iota(jnp.int32, (high_rows, 1), 0)
    line_f = lax.rem(line, slots)
    line_a = (line - line_f).astype(F32) * (1.0 / slots)
    slab_of = jnp.zeros((high_rows, 1), F32)
    for f in range(slots):
        mine = lane_sum(jnp.where(lane_r == f, xm, 0.0))
        slab = jnp.zeros((1, 1), F32)
        for k in range(1, n):
            slab = slab + jnp.where(mine >= k * bx, 1.0, 0.0)
        t = shifted + (slab - srcs)
        good = jnp.logical_or(t == 0, jnp.logical_or(t == n, t == -n))
        place = jnp.where(good, ext - (mine - slab * bx), FAR)
        hots.append(jnp.where(sub_w == place, 1.0, 0.0).astype(BF))
        slab_of = jnp.where(line_f == f, slab, slab_of)
    m = dot(tabi[...], jnp.concatenate(hots, axis=0))
    same = jnp.logical_and(line_a == inner, slab_of == srcs)
    mx[:high_rows] = jnp.where(same, 1.0, m[:high_rows]).astype(BF)
    mx[high_rows:] = m[high_rows:].astype(BF)
    for j in range(1, n):
        root_copy[j].wait_recv()
        matrices(j, rt.at[j])

    lane_h = lax.broadcasted_iota(jnp.int32, (pad, LANES), 1)
    blank = jnp.zeros((pad - by, LANES), F32)

    def full(v):
        return jnp.concatenate([v, blank], axis=0)

    def keep(x, c, side, v):
        h, l = split(v)
        lanes = slice(side * LANES, (side + 1) * LANES)
        yb[x, c * pad:(c + 1) * pad, lanes] = h
        yb[x, half + c * pad:half + (c + 1) * pad, lanes] = l

    def inner_row(c, block):
        def one(x, carry):
            keep(x, c, 0, full(block[x]))
            return carry
        return one

    def halo_row(x, carry):
        t = HALO * x // LANES
        at = HALO * x - LANES * t
        t_next = (HALO * x + HALO - 1) // LANES
        back = lax.rem(LANES - at, LANES)
        for c, halos in enumerate((zin, zpeer)):
            def piece(side, place):
                turn = lax.rem(back + place, LANES)
                one = pltpu.roll(full(halos[side, t]), turn, 1)
                two = pltpu.roll(full(halos[side, t_next]), turn, 1)
                return jnp.where(lane_h - place < LANES - at, one, two)
            second = jnp.where(lane_h < HALO, piece(1, 0), jnp.where(lane_h < 2 * HALO, piece(0, HALO), 0.0))
            keep(x, c, 1, second)
        return carry

    def row(p, x, s, group):
        first, count = (bank[0] * G, G) if group == [0] else (0, (n - 1) * G)
        m = slice(first, first + count)
        r = dot(lhs[p, m, :2 * half], yb[x]) + dot(lhs[p, m, 2 * half:], yb[x, :half])
        for side in range(2):
            us[side, pl.ds(first * 8 + s, count, stride=8), :] = r[:, side * LANES:(side + 1) * LANES]

    def finish(j, p):
        held = slice(bank[j] * G * 8, (bank[j] + 1) * G * 8)
        h, l = split(jnp.concatenate([us[0, held], us[1, held]], axis=1))
        a = dot(h, wz[j, p])
        return a[:, :LANES] + a[:, LANES:] + dot(l, wz[j, p, :, :LANES])

    def store(ref, j, at, r):
        for b in range(G):
            ref[j, pl.ds(at, 8), b * G:(b + 1) * G] = r[8 * b:8 * b + 8, :G]

    def sent(j, q):
        at = pl.ds(pl.multiple_of(8 * q, 8), 8)
        return copy(outb.at[j, at], got.at[j, at], gx_s.at[j, q], gx_r.at[j, q], other[j])

    def sent_mid(j):
        at = pl.ds(SIDES + 8, G)
        q = SIDES // 8 + 1
        return copy(outb.at[j, at], got.at[j, at], gx_s.at[j, q], gx_r.at[j, q], other[j])

    def emit(work, send, group):
        previous = None
        for j in group:
            work(j)
            if previous:
                send(previous).start()
            previous = j

    def side_octet(group, c0):
        def one(c, carry):
            p, x0 = octet_place(bx, 2 * c)
            for s in range(8):
                row(p, x0 + s, s, group)
            if group[-1]:
                @pl.when(c > c0)
                def _():
                    sent(group[-1], c - 1).start()
            emit(lambda j: store(outb, j, pl.multiple_of(8 * c, 8), finish(j, p)), lambda j: sent(j, c), group)
            return carry
        return one

    def mid_octet(group):
        def one(c, carry):
            for s in range(8):
                row(1, 8 * c + s, s, group)
            for j in group:
                store(mids, j, pl.multiple_of(8 * c, 8), finish(j, 1))
            return carry
        return one

    def tail_octet(group):
        for k, (p, x) in enumerate(tail):
            row(p, x, k, group)
        if group[-1]:
            sent(group[-1], SIDES // 8 - 1).start()

        def work(j):
            base = bank[j] * G * 8
            for p in range(3):
                spots = [pl.ds(base + k, G, stride=8) for k, t in enumerate(tail) if t[0] == p]
                both = [jnp.concatenate([us[side, at] for at in spots], axis=0) for side in range(2)]
                h, l = split(jnp.concatenate(both, axis=1))
                a = dot(h, wz[j, p])
                a = a[:, :LANES] + a[:, LANES:] + dot(l, wz[j, p, :, :LANES])
                for k, at in enumerate(spots):
                    us[0, at, :] = a[k * G:(k + 1) * G]
            total = us[0, base:base + G * 8]
            store(outb, j, SIDES, total)
            store(mids, j, MIDS - 8, total)

        emit(work, lambda j: sent(j, SIDES // 8), group)

    lax.fori_loop(0, bx, inner_row(0, pot), 0)
    for c in raw:
        c.wait_recv()
    lax.fori_loop(0, bx, inner_row(1, peer), 0)
    for c in zc[0]:
        c.wait_recv()
    for c in rel[0]:
        c.start()
    for s, (x0, x1, i0, i1, _, _) in enumerate(plan):
        for c in rel[s]:
            c.wait_recv()
        lax.fori_loop(x0, x1, halo_row, 0)
        c0, c1 = (i0 + 1) // 2, (i1 + 1) // 2
        lax.fori_loop(c0, c1, side_octet(order, c0), 0)
        if s < last:
            for c in zc[s + 1]:
                c.wait_recv()
            for c in rel[s + 1]:
                c.start()
            if c1 > c0:
                sent(order[-1], c1 - 1).start()
        else:
            tail_octet(order)
        lax.fori_loop(i0 // 2, i1 // 2, mid_octet(order), 0)

    tile = 2 * LANES
    tiles = G * G // tile

    def mid_work(j):
        def one(t, carry):
            at = pl.ds(pl.multiple_of(t * tile, tile), tile)
            h, l = split(mids[j, :, at])
            both = jnp.concatenate([h, l], axis=0)
            outb[j, SIDES + 8:SIDES + 8 + G, at] = (
                dot(ma[j, :, :2 * MIDS], both) + dot(ma[j, :, LANES:LANES + MIDS], h))
            return carry
        lax.fori_loop(0, tiles, one, 0)

    sent(order[-1], SIDES // 8).start()
    emit(mid_work, sent_mid, order)
    for s in range(8):
        row(2, s, s, [0])
    sent_mid(order[-1]).start()
    lax.fori_loop(0, SIDES // 8, side_octet([0], 0), 0)
    lax.fori_loop(0, octets // 2, mid_octet([0]), 0)
    tail_octet([0])
    mid_work(0)

    def gather_rows(first, rows, at):
        return jnp.concatenate([outb[0, first:first + rows, at]] + [got[j, first:first + rows, at]
                                                                    for j in range(1, n)], axis=0)

    def across(first, rows, k0, at):
        h, l = split(gather_rows(first, rows, at))
        both = dot(mx[:, k0:k0 + n * 64], h)
        return both[:high_rows] + both[high_rows:] + dot(mx[:high_rows, k0:k0 + n * 64], l)

    for s in range(last + 1):
        raw[s].wait_send()
        for c in zc[s] + rel[s]:
            c.wait_send()
    for j in range(1, n):
        root_copy[j].wait_send()

    def arrived(q, carry):
        for j in range(1, n):
            sent(j, q).wait()
        return carry

    lax.fori_loop(0, SIDES // 8, arrived, 0)

    def first_part(t, carry):
        at = pl.ds(pl.multiple_of(t * tile, tile), tile)
        acc[:, at] = across(0, SIDES, 0, at)
        return carry

    lax.fori_loop(0, tiles, first_part, 0)
    arrived(SIDES // 8, 0)
    for j in range(1, n):
        sent_mid(j).wait()

    def second_part(t, carry):
        at = pl.ds(pl.multiple_of(t * tile, tile), tile)
        r = acc[:, at] + across(SIDES, 64, n * 64, at)
        for a in range(G):
            where = pl.multiple_of(a * G * G + t * tile, LANES)
            out[:, pl.ds(where, tile)] = r[a * slots:(a + 1) * slots]
        return carry

    lax.fori_loop(0, tiles, second_part, 0)


def fused(info, pot, roots, consts):
    n, ny, nz, slots = info
    bx, by, bz = pot.shape
    octets = layout(bx)[3]
    chunks = len(CHUNKS)
    pad = -(-by // 16) * 16
    half = ny * pad
    dma = pltpu.SemaphoreType.DMA
    vmem = pl.BlockSpec(memory_space=pltpu.VMEM)
    folded = (2, tiles_of(bx), by, LANES)
    return pl.pallas_call(
        lambda *refs: fused_kernel(info, *refs),
        in_specs=[pl.BlockSpec(memory_space=pl.ANY)] + [vmem] * 5,
        out_specs=vmem,
        out_shape=jax.ShapeDtypeStruct((slots, G ** 3), F32),
        scratch_shapes=[
            pltpu.VMEM((bx, by, LANES), F32),
            pltpu.VMEM((n, BLOCK, G * G), F32),
            pltpu.VMEM((2 * G * slots, 2 * n * 64), BF),
            pltpu.VMEM((bx, by, LANES), F32),
            pltpu.VMEM(folded, F32),
            pltpu.VMEM(folded, F32),
            pltpu.VMEM(folded, F32),
            pltpu.VMEM((n, 8, LANES), F32),
            pltpu.VMEM((bx, 2 * half, 2 * LANES), BF),
            pltpu.VMEM((3, n * G, 3 * half), BF),
            pltpu.VMEM((n, 3, 2 * LANES, 2 * LANES), BF),
            pltpu.VMEM((2, n * G * 8, LANES), F32),
            pltpu.VMEM((n, BLOCK, G * G), F32),
            pltpu.VMEM((n, MIDS, G * G), F32),
            pltpu.VMEM((n, G, 2 * LANES), BF),
            pltpu.VMEM((G * slots, G * G), F32),
            dma((2,)), dma((chunks,)), dma((chunks,)),
            dma((2, chunks)), dma((2, chunks)),
            dma((2, chunks)), dma((2, chunks)),
            dma((n,)), dma((n,)),
            dma((n, SIDES // 8 + 2)), dma((n, SIDES // 8 + 2)),
        ],
        compiler_params=pltpu.CompilerParams(
            collective_id=0, has_side_effects=True, vmem_limit_bytes=56 * 1024 * 1024),
        cost_estimate=pl.CostEstimate(flops=24 * 10 ** 9, bytes_accessed=16 * 1024 * 1024, transcendentals=0),
        name="exchange_contract",
    )(pot, roots, *consts)


def body(potential, frag_root):
    bx, by, bz = potential.shape
    n, ny, nz = lax.axis_size("gx"), lax.axis_size("gy"), lax.axis_size("gz")
    slots = frag_root.shape[1]
    if n != 4:
        return plain_body(potential, frag_root)
    consts = [jnp.asarray(c) for c in tables(bx, n, slots)]
    return fused((n, ny, nz, slots), potential, frag_root, consts)


def solution(mesh):
    return jax.shard_map(
        body,
        mesh=mesh,
        in_specs=(P("gx", "gy", "gz"), P(None, ("gx", "gy", "gz"))),
        out_specs=P(("gx", "gy", "gz"), None),
        check_vma=False,
    )
```
